32 devices in a mesh: section: 2 (over x), row: 4 (over y, core), col: 4 (over z).
Axes of the slice: x: 2, y: 2, z: 4, core: 2. Of those that a mesh axis runs over, the one named last changes fastest.
Arguments:
- stash_inputs: bfloat16 [2, 4, 512, 12288], P('section', None, 'row', 'col'), may hold values from -16 to 16
- stash_hidden: bfloat16 [2, 4, 512, 24576], P('section', None, 'col', 'row'), may hold values from -6 to 6
- grad_in: bfloat16 [2, 512, 12288], P('section', 'row', 'col'), may hold values from -6 to 6
- w_in: bfloat16 [2, 12288, 24576], P('section', 'col', 'row'), may hold values from -0.0546875 to 0.0546875
- b_in: float32 [2, 24576], P('section', 'row'), may hold values from -3 to 3
- w_out: bfloat16 [2, 24576, 12288], P('section', 'row', 'col'), may hold values from -0.0390625 to 0.0390625
- b_out: float32 [2, 12288], P('section', 'col'), may hold values from -3 to 3
- ln_gain: float32 [2, 12288], P('section', 'col'), may hold values from 0.4 to 1.6
- plan: int32 [2, 2], P('section'), may hold values from 0 to 3, as said below
Outputs:
- act_recv: bfloat16 [2, 512, 12288], P('section', 'row', 'col')
- grad_recv: bfloat16 [2, 512, 12288], P('section', 'row', 'col')
- saved_hidden: bfloat16 [2, 512, 24576], P('section', 'col', 'row')
The draws below stay inside these ranges and needn't reach their ends.
Inputs may be any that keep to these rules, and one draw needn't show every extreme that they name: plan[s, 0] is the stash slot of the micro-batch that section s takes backward, plan[s, 1] that of the one it takes forward; the two differ.
All inputs are finite; a program needn't handle non-finite values.
Results may differ from the reference program's by a relative error of at most 0.015.
Values may be sent and summed in bfloat16 or wider, within the bound.
A program may use at most 192 MiB of HBM per device.

```python
import jax
import jax.numpy as jnp
from jax import lax

D = 12288
FF = 24576
TOK = 512
STASH = 4
N_SECTION = 2


def draw_stash_inputs(key, part):
    key_noise = jax.random.fold_in(key, 11)
    key_cols = jax.random.fold_in(key, 12)
    ramp = jnp.arange(D, dtype=jnp.float32) / D
    col_scale = jnp.exp(ramp * jnp.log(3.0) + jax.random.uniform(key_cols, (D,), jnp.float32, 0.0, jnp.log(4.0))) / 6.0
    noise = jnp.clip(jax.random.normal(key_noise, (N_SECTION, STASH, TOK, D), jnp.float32), -6.0, 6.0)
    values = noise * col_scale
    return values.astype(jnp.bfloat16)


def draw_plan(key, part):
    key_back = jax.random.fold_in(key, 21)
    key_step = jax.random.fold_in(key, 22)
    back_slot = jax.random.randint(key_back, (N_SECTION,), 0, STASH)
    step_size = jax.random.randint(key_step, (N_SECTION,), 1, STASH)
    fwd_slot = (back_slot + step_size) % STASH
    return jnp.stack([back_slot, fwd_slot], axis=1).astype(jnp.int32)


def levels(own_key, dims, pieces, smallest, largest):
    level = 1.0
    for dim, shards_of in pieces:
        steps = jax.random.uniform(jax.random.fold_in(jax.random.fold_in(own_key, 6), dim), (shards_of,), jnp.float32, smallest / len(pieces), largest / len(pieces))
        level = level * jnp.repeat(jnp.exp(steps), dims[dim] // shards_of).reshape((-1,) + (1,) * (len(dims) - 1 - dim))
    return level


def scatter_about(rng, shape, width, limit, pieces=(), held_as=jnp.bfloat16):
    drawn = jax.random.normal(rng, shape, jnp.float32) * width
    if len(pieces) > 0:
        drawn = levels(rng, shape, pieces, -0.22, 0.18) * drawn
    return jnp.clip(drawn, min=-limit, max=limit).astype(held_as)


def setup_inputs(seed: int = 0) -> dict:
    arg_keys = jax.random.split(jax.random.key(seed), 10)
    return {
        "stash_inputs": draw_stash_inputs(jax.random.fold_in(arg_keys[9], 71), 0),
        "stash_hidden": scatter_about(arg_keys[1], (N_SECTION, STASH, TOK, FF), 1.5, 6.0, ((0, 2), (2, 4), (3, 4))),
        "grad_in": scatter_about(arg_keys[2], (N_SECTION, TOK, D), 1.0, 6.0, ((0, 2), (1, 4), (2, 4))),
        "w_in": scatter_about(arg_keys[3], (N_SECTION, D, FF), D ** -0.5, 0.0546875, ((0, 2), (1, 4), (2, 4))),
        "b_in": scatter_about(arg_keys[4], (N_SECTION, FF), 0.5, 3.0, ((0, 2), (1, 4)), jnp.float32),
        "w_out": scatter_about(arg_keys[5], (N_SECTION, FF, D), FF ** -0.5, 0.0390625, ((0, 2), (1, 4), (2, 4))),
        "b_out": scatter_about(arg_keys[6], (N_SECTION, D), 0.5, 3.0, ((0, 2), (1, 4)), jnp.float32),
        "ln_gain": jnp.clip(1.0 + 0.12 * jax.random.normal(arg_keys[7], (N_SECTION, D), jnp.float32), 0.4, 1.6),
        "plan": draw_plan(jax.random.fold_in(arg_keys[9], 71), 0),
    }


epsilon = 1e-05
root_coef = 0.7978845608028654
cubic_coef = 0.044715

def gelu_value(values):
    inner = root_coef * (values + cubic_coef * values * values * values)
    return 0.5 * values * (1.0 + jnp.tanh(inner))

def gelu_slope(values):
    inner = root_coef * (values + cubic_coef * values * values * values)
    tangent = jnp.tanh(inner)
    return 0.5 * (1.0 + tangent) + 0.5 * values * (1.0 - tangent * tangent) * root_coef * (1.0 + 3.0 * cubic_coef * values * values)

def finish_norm(values, total, squares):
    mean_val = total / D
    sq_mean = squares / D
    inv_std = lax.rsqrt(sq_mean - mean_val * mean_val + epsilon)
    return ((values - mean_val[:, None]) * inv_std[:, None], inv_std)

def transposed(left, right):
    return lax.dot_general(left, right, (((1,), (1,)), ((), ())), preferred_element_type=jnp.float32)

def section_step(fwd_input, bwd_input, bwd_hidden, upstream, w_first, b_first, w_second, b_second, gain_part):
    fwd_hat, fwd_inv = finish_norm(fwd_input, lax.optimization_barrier(jnp.sum(fwd_input, axis=1)), lax.optimization_barrier(jnp.sum(fwd_input * fwd_input, axis=1)))
    bwd_hat, bwd_inv = finish_norm(bwd_input, lax.optimization_barrier(jnp.sum(bwd_input, axis=1)), lax.optimization_barrier(jnp.sum(bwd_input * bwd_input, axis=1)))
    normed = (fwd_hat * gain_part).astype(jnp.bfloat16)
    hidden = jnp.dot(normed, w_first, preferred_element_type=jnp.float32) + b_first
    saved = hidden.astype(jnp.bfloat16)
    activated = gelu_value(hidden).astype(jnp.bfloat16)
    output = (jnp.dot(activated, w_second, preferred_element_type=jnp.float32) + b_second + fwd_input).astype(jnp.bfloat16)
    slopes = transposed(upstream, w_second)
    hid_grad = (slopes * gelu_slope(bwd_hidden)).astype(jnp.bfloat16)
    scaled = transposed(hid_grad, w_first) * gain_part
    first_mean = lax.optimization_barrier(jnp.sum(scaled, axis=1)) / D
    second_mean = lax.optimization_barrier(jnp.sum(scaled * bwd_hat, axis=1)) / D
    in_grad = upstream.astype(jnp.float32) + bwd_inv[:, None] * (scaled - first_mean[:, None] - bwd_hat * second_mean[:, None])
    return (output, in_grad.astype(jnp.bfloat16), saved)

def reference(stash_inputs, stash_hidden, grad_in, w_in, b_in, w_out, b_out, ln_gain, plan):
    outputs = []
    grads = []
    saves = []
    for section_id in range(N_SECTION):
        bwd_slot = plan[section_id, 0]
        fwd_slot = plan[section_id, 1]
        fwd_input = lax.dynamic_index_in_dim(stash_inputs[section_id], fwd_slot, 0, keepdims=False).astype(jnp.float32)
        bwd_input = lax.dynamic_index_in_dim(stash_inputs[section_id], bwd_slot, 0, keepdims=False).astype(jnp.float32)
        bwd_hidden = lax.dynamic_index_in_dim(stash_hidden[section_id], bwd_slot, 0, keepdims=False).astype(jnp.float32)
        output, in_grad, saved = section_step(fwd_input, bwd_input, bwd_hidden, grad_in[section_id], w_in[section_id], b_in[section_id], w_out[section_id], b_out[section_id], ln_gain[section_id])
        outputs.append(output)
        grads.append(in_grad)
        saves.append(saved)
    act_recv = jnp.stack([outputs[(section_id - 1) % N_SECTION] for section_id in range(N_SECTION)])
    grad_recv = jnp.stack([grads[(section_id + 1) % N_SECTION] for section_id in range(N_SECTION)])
    return (act_recv, grad_recv, jnp.stack(saves))
```

```python
import functools

import jax
import jax.numpy as jnp
from jax import lax
from jax.experimental import pallas as pl
from jax.experimental.pallas import tpu as pltpu
from jax.sharding import PartitionSpec as P

MESH = pl.DeviceIdType.MESH
F32 = jnp.float32
BF16 = jnp.bfloat16
LANE = 128
EPSILON = 1e-05
ROOT = 0.7978845608028654
CUBIC = 0.044715
WIDTH = 512
STRIP = 256


def gelu_value(values):
    inner = ROOT * (values + CUBIC * values * values * values)
    return 0.5 * values * (1.0 + jnp.tanh(inner))


def gelu_slope(values):
    inner = ROOT * (values + CUBIC * values * values * values)
    tangent = jnp.tanh(inner)
    return 0.5 * (1.0 + tangent) + 0.5 * values * (1.0 - tangent * tangent) * ROOT * (
        1.0 + 3.0 * CUBIC * values * values
    )


def flipped(index, bit):
    return index + bit * (1 - 2 * ((index // bit) % 2))


def flipped_by(index, mask):
    bit = 1
    while bit <= mask:
        if mask & bit:
            index = flipped(index, bit)
        bit *= 2
    return index


def strips(columns, strip, body):
    @pl.loop(0, columns // strip)
    def _(step):
        body(pl.ds(pl.multiple_of(step * strip, strip), strip))


def kernel(
    n, ranks, sections, width, pieces,
    fwd_in, bwd_in, bwd_hidden, upstream, b_in, b_out, gain, w_in, w_out,
    act_recv, grad_recv, saved,
    up_all, normed_all, acc, first_in, first_out, second_in, second_out,
    part, moved, held, total, own, stats, stat_sent, stat_got,
    half_sent, half_got, side_sent, side_got, final,
    first_sem, second_sem, sum_send, sum_recv, spread_send, spread_recv,
    gather_send, gather_recv, stat_send, stat_recv,
    half_send, half_recv, side_send, side_recv, final_send, final_recv,
    credit, half_free, side_free,
):
    col = lax.axis_index("col")
    row = lax.axis_index("row")
    section = lax.axis_index("section")
    tokens, features = up_all.shape
    hidden_units = w_in.shape[1]
    own_rows = tokens // ranks
    block = tokens // n
    chunks = hidden_units // width
    queue = 2 * chunks
    piece = features // pieces
    side = ranks // 2
    last = n - 1
    inverse = 1.0 / (features * n)
    strip = min(STRIP, features)

    barrier = pltpu.get_barrier_semaphore()
    for away in range(1, n):
        pl.semaphore_signal(barrier, 1, device_id={"col": (col + away) % n}, device_id_type=MESH)
    pl.semaphore_signal(barrier, 1, device_id={"row": flipped(row, 1)}, device_id_type=MESH)
    pl.semaphore_signal(barrier, 1, device_id={"row": flipped(row, side)}, device_id_type=MESH)
    for away in (1, sections - 1):
        pl.semaphore_signal(
            barrier, 1, device_id={"section": (section + away) % sections}, device_id_type=MESH
        )
    pl.semaphore_wait(barrier, n - 1 + 2 + 2)

    def rows_of(index):
        return pl.ds(pl.multiple_of(index * own_rows, own_rows), own_rows)

    def block_of(index):
        return pl.ds(pl.multiple_of(index * block, block), block)

    def gather_copy(which, source, target, index, hop):
        bit = side if hop == 0 else 1
        place = rows_of(index)
        return pltpu.make_async_remote_copy(
            src_ref=source if source is not None else target.at[place],
            dst_ref=target.at[place],
            send_sem=gather_send.at[which, hop],
            recv_sem=gather_recv.at[which, hop],
            device_id={"row": flipped(row, bit)},
            device_id_type=MESH,
        )

    gather_copy(0, upstream, up_all, row, 0).start()
    gather_copy(0, upstream, up_all, row, 1).start()

    def take_up(cols):
        up_all[rows_of(row), cols] = upstream[:, cols]
        acc[:, cols] = jnp.zeros((tokens, cols.size), F32)

    def first_copy(index, start):
        slot = lax.rem(index, 2)

        @pl.when(index < chunks)
        def _():
            place = pl.ds(pl.multiple_of(index * width, width), width)
            copy = pltpu.make_async_copy(w_out.at[place], first_out.at[slot], first_sem.at[slot])
            copy.start() if start else copy.wait()

        @pl.when(index >= chunks)
        def _():
            place = pl.ds(pl.multiple_of((index - chunks) * width, width), width)
            copy = pltpu.make_async_copy(w_in.at[:, place], first_in.at[slot], first_sem.at[slot])
            copy.start() if start else copy.wait()

    def second_copy(index, start):
        slot = lax.rem(index, 2)

        @pl.when(index < chunks)
        def _():
            place = pl.ds(pl.multiple_of(index * width, width), width)
            copy = pltpu.make_async_copy(w_in.at[:, place], second_in.at[slot], second_sem.at[slot])
            copy.start() if start else copy.wait()

        @pl.when(index >= chunks)
        def _():
            place = pl.ds(pl.multiple_of((index - chunks) * width, width), width)
            copy = pltpu.make_async_copy(w_out.at[place], second_out.at[slot], second_sem.at[slot])
            copy.start() if start else copy.wait()

    first_copy(jnp.int32(0), True)
    second_copy(jnp.int32(0), True)
    strips(features, strip, take_up)

    lane = lax.broadcasted_iota(jnp.int32, (own_rows, LANE), 1)

    def packed(columns):
        values = jnp.zeros((own_rows, LANE), F32)
        for place, column in enumerate(columns):
            values = jnp.where(lane == place, column, values)
        return values

    def stat_copy(which, away):
        return pltpu.make_async_remote_copy(
            src_ref=stat_sent.at[which],
            dst_ref=stat_got.at[which, away - 1],
            send_sem=stat_send.at[which, away - 1],
            recv_sem=stat_recv.at[which, away - 1],
            device_id={"col": (col + away) % n},
            device_id_type=MESH,
        )

    def summed(which):
        values = stat_sent[which]
        for away in range(1, n):
            stat_copy(which, away).wait_recv()
            values = values + stat_got[which, away - 1]
        return values

    def reduced(source):
        def one(step, sums):
            cols = pl.ds(pl.multiple_of(step * strip, strip), strip)
            values = source(cols)
            return tuple(
                s + jnp.sum(v, axis=1, keepdims=True) for s, v in zip(sums, values, strict=True)
            )

        zero = jnp.zeros((own_rows, 1), F32)
        return lax.fori_loop(0, features // strip, one, (zero,) * 2)

    def moments(ref):
        def source(cols):
            values = ref[:, cols].astype(F32)
            return values, values * values

        return reduced(source)

    stat_sent[0] = packed(moments(fwd_in) + moments(bwd_in))
    for away in range(1, n):
        stat_copy(0, away).start()
    sums = summed(0)

    def scale_of(total_sum, squares):
        mean = total_sum * inverse
        return mean, lax.rsqrt(squares * inverse - mean * mean + EPSILON)

    stats[...] = packed(
        scale_of(sums[:, 0:1], sums[:, 1:2]) + scale_of(sums[:, 2:3], sums[:, 3:4])
    )

    def normalize(cols):
        hat = (fwd_in[:, cols].astype(F32) - stats[:, 0:1]) * stats[:, 1:2]
        normed_all[rows_of(row), cols] = (hat * gain[:, cols]).astype(BF16)

    strips(features, strip, normalize)
    gather_copy(1, None, normed_all, row, 0).start()
    gather_copy(1, None, normed_all, row, 1).start()

    def pass_on(which, target):
        far = flipped(row, side)
        gather_copy(which, None, target, far, 0).wait_recv()
        gather_copy(which, None, target, far, 2).start()

    def gathered(which, target):
        near = flipped(row, 1)
        gather_copy(which, None, target, near, 1).wait_recv()
        gather_copy(which, None, target, flipped(near, side), 2).wait_recv()
        for hop in range(3):
            gather_copy(which, None, target, row, hop).wait_send()

    pass_on(0, up_all)
    gathered(0, up_all)

    def neighbour(way):
        return jnp.minimum(col + 1, last) if way == 0 else jnp.maximum(col - 1, 0)

    def place_in_line(way):
        return col if way == 0 else last - col

    def sum_copy(way, index, hop, target):
        return pltpu.make_async_remote_copy(
            src_ref=part.at[lax.rem(index, n), block_of(target)],
            dst_ref=moved.at[way, lax.rem(index, 3), hop],
            send_sem=sum_send.at[way, lax.rem(index + hop, 2), hop],
            recv_sem=sum_recv.at[way, lax.rem(index, 3), hop],
            device_id={"col": neighbour(way)},
            device_id_type=MESH,
        )

    def spread_copy(way, index, hop, origin):
        slot = lax.rem(index, n + 1)
        return pltpu.make_async_remote_copy(
            src_ref=held.at[slot, block_of(origin)],
            dst_ref=held.at[slot, block_of(origin)],
            send_sem=spread_send.at[way, lax.rem(index + hop, 2), hop],
            recv_sem=spread_recv.at[way, lax.rem(index, 3), hop],
            device_id={"col": neighbour(way)},
            device_id_type=MESH,
        )

    def valid(index):
        return jnp.logical_and(index >= 0, index < queue)

    def sum_target(way, hop):
        at = last - hop + place_in_line(way)
        return at if way == 0 else last - at

    def spread_origin(way, hop):
        return col - hop if way == 0 else col + hop

    def sum_step(index, hop):
        for way in range(2):
            at = place_in_line(way)

            @pl.when(valid(index) & (at <= hop) & (at < last))
            def _():
                target = sum_target(way, hop)
                if hop > 0:

                    @pl.when(at > 0)
                    def _():
                        sum_copy(way, index, hop - 1, target).wait_recv()
                        slot = lax.rem(index, n)
                        mine = part[slot, block_of(target)].astype(F32)
                        more = moved[way, lax.rem(index, 3), hop - 1].astype(F32)
                        part[slot, block_of(target)] = (mine + more).astype(BF16)

                sum_copy(way, index, hop, target).start()

    def sum_sent(index, hop):
        for way in range(2):
            at = place_in_line(way)

            @pl.when(valid(index) & (at <= hop) & (at < last))
            def _():
                sum_copy(way, index, hop, sum_target(way, hop)).wait_send()

    def spread_step(index, hop):
        for way in range(2):
            at = place_in_line(way)

            @pl.when(valid(index) & (at >= hop))
            def _():
                origin = spread_origin(way, hop)
                if hop > 0:
                    spread_copy(way, index, hop - 1, origin).wait_recv()

                @pl.when(at < last)
                def _():
                    spread_copy(way, index, hop, origin).start()

    def spread_sent(index, hop):
        for way in range(2):
            at = place_in_line(way)

            @pl.when(valid(index) & (at >= hop) & (at < last))
            def _():
                spread_copy(way, index, hop, spread_origin(way, hop)).wait_send()

    def spread_done(index):
        for way in range(2):

            @pl.when(place_in_line(way) == last)
            def _():
                spread_copy(way, index, n - 2, spread_origin(way, last)).wait_recv()

    def activate(index):
        slot = lax.rem(index, n)
        out_slot = lax.rem(index, n + 1)
        for way in range(2):

            @pl.when(place_in_line(way) > 0)
            def _():
                sum_copy(way, index, n - 2, col).wait_recv()

        total[...] = part[slot, block_of(col)].astype(F32)
        for way in range(2):

            @pl.when(place_in_line(way) > 0)
            def _():
                total[...] += moved[way, lax.rem(index, 3), n - 2].astype(F32)

        tile = min(STRIP, width)

        @pl.when(index < chunks)
        def _():
            for at in range(0, width, tile):
                cols = pl.ds(pl.multiple_of(index * width + at, tile), tile)
                slope = gelu_slope(bwd_hidden[:, cols].astype(F32))
                held[out_slot, block_of(col), at : at + tile] = (
                    total[:, at : at + tile] * slope
                ).astype(BF16)

        @pl.when(index >= chunks)
        def _():
            for at in range(0, width, tile):
                cols = pl.ds(pl.multiple_of((index - chunks) * width + at, tile), tile)
                values = total[:, at : at + tile] + b_in[:, cols]
                saved[:, cols] = values.astype(BF16)
                held[out_slot, block_of(col), at : at + tile] = gelu_value(values).astype(BF16)

    both_last = (((1,), (1,)), ((), ()))
    both_inner = (((1,), (0,)), ((), ()))

    def first_product(index):
        slot = lax.rem(index, 2)
        out_slot = lax.rem(index, n)
        tile = min(256, width)

        @pl.when(index < chunks)
        def _():
            for at in range(0, width, tile):
                part[out_slot, :, at : at + tile] = lax.dot_general(
                    up_all[...], first_out[slot, at : at + tile, :], both_last,
                    preferred_element_type=F32,
                ).astype(BF16)

        @pl.when(index >= chunks)
        def _():
            for at in range(0, width, tile):
                part[out_slot, :, at : at + tile] = lax.dot_general(
                    normed_all[...], first_in[slot, :, at : at + tile], both_inner,
                    preferred_element_type=F32,
                ).astype(BF16)

    def second_product(index):
        slot = lax.rem(index, 2)
        in_slot = lax.rem(index, n + 1)
        tile = min(256, features)
        group = 2 if features % (2 * tile) == 0 else 1

        @pl.when(index < chunks)
        def _():
            @pl.loop(0, features // (tile * group))
            def _(step):
                for k in range(group):
                    at = pl.ds(pl.multiple_of((step * group + k) * tile, tile), tile)
                    acc[:, at] += lax.dot_general(
                        held[in_slot], second_in[slot, at, :], both_last,
                        preferred_element_type=F32,
                    )

        @pl.when(index >= chunks)
        def _():
            @pl.loop(0, features // (tile * group))
            def _(step):
                for k in range(group):
                    at = pl.ds(pl.multiple_of((step * group + k) * tile, tile), tile)
                    acc[:, at] += lax.dot_general(
                        held[in_slot], second_out[slot, :, at], both_inner,
                        preferred_element_type=F32,
                    )

    def half_copy(which, k):
        return pltpu.make_async_remote_copy(
            src_ref=half_sent.at[k],
            dst_ref=half_got.at[k],
            send_sem=half_send.at[which, k],
            recv_sem=half_recv.at[which, k],
            device_id={"row": flipped(row, 1)},
            device_id_type=MESH,
        )

    def side_copy(which, p):
        return pltpu.make_async_remote_copy(
            src_ref=side_sent.at[p],
            dst_ref=side_got.at[p],
            send_sem=side_send.at[which, p],
            recv_sem=side_recv.at[which, p],
            device_id={"row": flipped(row, side)},
            device_id_type=MESH,
        )

    def final_copy(which, p):
        target = grad_recv if which == 0 else act_recv
        away = sections - 1 if which == 0 else 1
        cols = pl.ds(p * piece, piece)
        return pltpu.make_async_remote_copy(
            src_ref=final.at[which, :, cols],
            dst_ref=target.at[:, cols],
            send_sem=final_send.at[which, p],
            recv_sem=final_recv.at[which, p],
            device_id={"section": (section + away) % sections},
            device_id_type=MESH,
        )

    def fold_near(which):
        if which == 1:
            pl.semaphore_wait(half_free, 1)
        for k in (1, 0):
            index = flipped_by(row, 1 + side * k)

            def cut(cols):
                half_sent[k, :, cols] = acc[rows_of(index), cols].astype(BF16)

            strips(features, strip, cut)
            half_copy(which, k).start()

    def fold_far(which):
        half_copy(which, 1).wait_recv()
        if which == 1:
            pl.semaphore_wait(side_free, 1)
        far = flipped(row, side)
        for p in range(pieces):
            cols = pl.ds(p * piece, piece)
            side_sent[p] = (
                acc[rows_of(far), cols] + half_got[1, :, cols].astype(F32)
            ).astype(BF16)
            side_copy(which, p).start()
        half_copy(which, 0).wait_recv()

        def keep(cols):
            own[:, cols] = acc[rows_of(row), cols] + half_got[0, :, cols].astype(F32)

        strips(features, strip, keep)
        for k in range(2):
            half_copy(which, k).wait_send()
        if which == 0:
            pl.semaphore_signal(
                half_free, 1, device_id={"row": flipped(row, 1)}, device_id_type=MESH
            )

            def clear(cols):
                acc[:, cols] = jnp.zeros((tokens, cols.size), F32)

            strips(features, strip, clear)

    def backward_hat(cols):
        return (bwd_in[:, cols].astype(F32) - stats[:, 2:3]) * stats[:, 3:4]

    def backward_sums():
        for p in range(pieces):
            side_copy(0, p).wait_recv()
            cols = pl.ds(p * piece, piece)
            own[:, cols] = (own[:, cols] + side_got[p].astype(F32)) * gain[:, cols]
        for p in range(pieces):
            side_copy(0, p).wait_send()
        pl.semaphore_signal(
            side_free, 1, device_id={"row": flipped(row, side)}, device_id_type=MESH
        )

        def source(cols):
            scaled = own[:, cols]
            return scaled, scaled * backward_hat(cols)

        stat_sent[1] = packed(reduced(source))
        for away in range(1, n):
            stat_copy(1, away).start()

    def backward_end():
        sums = summed(1) * inverse
        stats[...] = packed((stats[:, 0:1], stats[:, 1:2], stats[:, 2:3], stats[:, 3:4], sums[:, 0:1], sums[:, 1:2]))

        def finish(cols):
            values = own[:, cols] - stats[:, 4:5] - backward_hat(cols) * stats[:, 5:6]
            final[0, :, cols] = (
                upstream[:, cols].astype(F32) + stats[:, 3:4] * values
            ).astype(BF16)

        strips(features, strip, finish)
        for p in range(pieces):
            final_copy(0, p).start()

    turn = 2 * n - 2
    steps = queue + turn
    middle = chunks - 1 + turn

    def step(m, carry):
        first_ready = valid(m)
        second = m - turn

        for way in range(2):

            @pl.when((m >= 2) & (place_in_line(way) < last))
            def _():
                pl.semaphore_wait(credit.at[way], 1)

        @pl.when(m + 1 < queue)
        def _():
            first_copy(m + 1, True)

        @pl.when((second + 1 >= 1) & (second + 1 < queue))
        def _():
            second_copy(second + 1, True)

        for hop in range(1, n - 1):
            sum_step(m - hop, hop)

        @pl.when(valid(m - last))
        def _():
            activate(m - last)

        for hop in range(n - 1):
            spread_step(m - last - hop, hop)

        @pl.when(m == min(4, chunks - 1))
        def _():
            pass_on(1, normed_all)

        @pl.when(m == chunks)
        def _():
            gathered(1, normed_all)

        @pl.when(first_ready)
        def _():
            first_copy(m, False)
            first_product(m)

        sum_step(m, 0)

        @pl.when(m == middle + 1)
        def _():
            fold_far(0)

        @pl.when(m == middle + 3)
        def _():
            backward_sums()

        @pl.when(m == middle + 4)
        def _():
            backward_end()

        @pl.when(valid(second))
        def _():
            spread_done(second)
            second_copy(second, False)
            second_product(second)

        @pl.when(m == middle)
        def _():
            fold_near(0)

        for hop in range(n - 1):
            sum_sent(m - 1 - hop, hop)
            spread_sent(m - 1 - last - hop, hop)

        for way in range(2):

            @pl.when((m < steps - 2) & (place_in_line(way) > 0))
            def _():
                pl.semaphore_signal(
                    credit.at[way], 1, device_id={"col": neighbour(1 - way)}, device_id_type=MESH
                )

        return carry

    lax.fori_loop(0, steps, step, 0)

    fold_near(1)
    fold_far(1)
    for p in range(pieces):
        cols = pl.ds(p * piece, piece)
        side_copy(1, p).wait_recv()
        final[1, :, cols] = (
            own[:, cols] + side_got[p].astype(F32) + b_out[:, cols] + fwd_in[:, cols].astype(F32)
        ).astype(BF16)
        final_copy(1, p).start()
    for p in range(pieces):
        side_copy(1, p).wait_send()
    for which in range(2):
        for away in range(1, n):
            stat_copy(which, away).wait_send()
        for p in range(pieces):
            final_copy(which, p).wait()


def cut_count(features):
    return max(p for p in range(1, 5) if features % (p * LANE) == 0)


def whole_layer(shape, *operands):
    n, ranks, sections = shape["col"], shape["row"], shape["section"]
    fwd_in, w_in = operands[0], operands[7]
    own_rows, features = fwd_in.shape
    hidden_units = w_in.shape[1]
    tokens = own_rows * ranks
    block = tokens // n
    width = WIDTH if n <= 8 else WIDTH // 2
    pieces = cut_count(features)
    dma = pltpu.SemaphoreType.DMA
    in_vmem = pl.BlockSpec(memory_space=pltpu.VMEM)
    anywhere = pl.BlockSpec(memory_space=pl.ANY)
    scratch = [
        pltpu.VMEM((tokens, features), BF16),
        pltpu.VMEM((tokens, features), BF16),
        pltpu.VMEM((tokens, features), F32),
        pltpu.VMEM((2, features, width), BF16),
        pltpu.VMEM((2, width, features), BF16),
        pltpu.VMEM((2, features, width), BF16),
        pltpu.VMEM((2, width, features), BF16),
        pltpu.VMEM((n, tokens, width), BF16),
        pltpu.VMEM((2, 3, n - 1, block, width), BF16),
        pltpu.VMEM((n + 1, tokens, width), BF16),
        pltpu.VMEM((block, width), F32),
        pltpu.VMEM((own_rows, features), F32),
        pltpu.VMEM((own_rows, LANE), F32),
        pltpu.VMEM((2, own_rows, LANE), F32),
        pltpu.VMEM((2, n - 1, own_rows, LANE), F32),
        pltpu.VMEM((2, own_rows, features), BF16),
        pltpu.VMEM((2, own_rows, features), BF16),
        pltpu.VMEM((pieces, own_rows, features // pieces), BF16),
        pltpu.VMEM((pieces, own_rows, features // pieces), BF16),
        pltpu.VMEM((2, own_rows, features), BF16),
        dma((2,)),
        dma((2,)),
        dma((2, 2, n - 1)),
        dma((2, 3, n - 1)),
        dma((2, 2, n - 1)),
        dma((2, 3, n - 1)),
        dma((2, 3)),
        dma((2, 3)),
        dma((2, n - 1)),
        dma((2, n - 1)),
        dma((2, 2)),
        dma((2, 2)),
        dma((2, pieces)),
        dma((2, pieces)),
        dma((2, pieces)),
        dma((2, pieces)),
        pltpu.SemaphoreType.REGULAR((2,)),
        pltpu.SemaphoreType.REGULAR,
        pltpu.SemaphoreType.REGULAR,
    ]
    return pl.pallas_call(
        functools.partial(kernel, n, ranks, sections, width, pieces),
        out_shape=(
            jax.ShapeDtypeStruct((own_rows, features), BF16),
            jax.ShapeDtypeStruct((own_rows, features), BF16),
            jax.ShapeDtypeStruct((block, hidden_units), BF16),
        ),
        in_specs=[in_vmem] * 7 + [anywhere] * 2,
        out_specs=(anywhere, anywhere, in_vmem),
        scratch_shapes=scratch,
        name="layer",
        cost_estimate=pl.CostEstimate(
            flops=8 * tokens * features * hidden_units,
            bytes_accessed=8 * features * hidden_units,
            transcendentals=0,
        ),
        compiler_params=pltpu.CompilerParams(
            collective_id=0, has_side_effects=True, vmem_limit_bytes=67043328
        ),
    )(*operands)


def body(shape, stash_inputs, stash_hidden, grad_in, w_in, b_in, w_out, b_out, ln_gain, plan):
    def picked(stash, slot):
        return lax.dynamic_index_in_dim(stash[0], slot, 0, keepdims=False)

    bwd_slot = plan[0, 0]
    fwd_slot = plan[0, 1]
    act, grad, saved = whole_layer(
        shape,
        picked(stash_inputs, fwd_slot),
        picked(stash_inputs, bwd_slot),
        picked(stash_hidden, bwd_slot),
        grad_in[0],
        b_in,
        b_out,
        ln_gain,
        w_in[0],
        w_out[0],
    )
    return (act[None], grad[None], saved[None])


def solution(mesh):
    in_specs = (
        P("section", None, "row", "col"),
        P("section", None, "col", "row"),
        P("section", "row", "col"),
        P("section", "col", "row"),
        P("section", "row"),
        P("section", "row", "col"),
        P("section", "col"),
        P("section", "col"),
        P("section", None),
    )
    out_specs = (P("section", "row", "col"), P("section", "row", "col"), P("section", "col", "row"))
    return jax.shard_map(
        functools.partial(body, dict(mesh.shape)),
        mesh=mesh,
        in_specs=in_specs,
        out_specs=out_specs,
        check_vma=False,
    )
```

```python
import functools

import jax
import jax.numpy as jnp
from jax import lax
from jax.experimental import pallas as pl
from jax.experimental.pallas import tpu as pltpu
from jax.sharding import PartitionSpec as P

MESH = pl.DeviceIdType.MESH
F32 = jnp.float32
BF16 = jnp.bfloat16
LANE = 128
EPSILON = 1e-05
ROOT = 0.7978845608028654
CUBIC = 0.044715
WIDTH = 384
STRIP = 256


def gelu_value(values):
    inner = ROOT * (values + CUBIC * values * values * values)
    return 0.5 * values * (1.0 + jnp.tanh(inner))


def gelu_slope(values):
    inner = ROOT * (values + CUBIC * values * values * values)
    tangent = jnp.tanh(inner)
    return 0.5 * (1.0 + tangent) + 0.5 * values * (1.0 - tangent * tangent) * ROOT * (
        1.0 + 3.0 * CUBIC * values * values
    )


def flipped(index, bit):
    return index + bit * (1 - 2 * ((index // bit) % 2))


def flipped_by(index, mask):
    bit = 1
    while bit <= mask:
        if mask & bit:
            index = flipped(index, bit)
        bit *= 2
    return index


def strips(columns, strip, body):
    @pl.loop(0, columns // strip)
    def _(step):
        body(pl.ds(pl.multiple_of(step * strip, strip), strip))


def kernel(
    n, ranks, sections, width, pieces,
    plan, b_in, b_out, gain, stash_inputs, stash_hidden, upstream, w_in, w_out,
    act_recv, grad_recv, saved,
    up_all, normed_all, acc, first_in, first_out, second_in, second_out,
    part, moved, held, total, own, stats, stat_sent, stat_got,
    half_sent, half_got, side_sent, side_got, final, kept, slopes,
    start_sem, slope_sem, first_sem, second_sem, sum_send, sum_recv, spread_send, spread_recv,
    gather_send, gather_recv, stat_send, stat_recv,
    half_send, half_recv, side_send, side_recv, final_send, final_recv,
    credit, half_free, side_free,
):
    col = lax.axis_index("col")
    row = lax.axis_index("row")
    section = lax.axis_index("section")
    tokens, features = up_all.shape
    hidden_units = w_in.shape[1]
    own_rows = tokens // ranks
    block = tokens // n
    chunks = hidden_units // width
    queue = 2 * chunks
    bwd_slot = plan[0, 0]
    fwd_slot = plan[0, 1]
    piece = features // pieces
    side = ranks // 2
    last = n - 1
    inverse = 1.0 / (features * n)
    strip = min(STRIP, features)

    barrier = pltpu.get_barrier_semaphore()
    for away in range(1, n):
        pl.semaphore_signal(barrier, 1, device_id={"col": (col + away) % n}, device_id_type=MESH)
    pl.semaphore_signal(barrier, 1, device_id={"row": flipped(row, 1)}, device_id_type=MESH)
    pl.semaphore_signal(barrier, 1, device_id={"row": flipped(row, side)}, device_id_type=MESH)
    for away in (1, sections - 1):
        pl.semaphore_signal(
            barrier, 1, device_id={"section": (section + away) % sections}, device_id_type=MESH
        )
    pl.semaphore_wait(barrier, n - 1 + 2 + 2)

    def chunk_of(unit):
        return lax.rem(unit, chunks)

    def backward(unit):
        return unit < chunks

    def fwd_in(cols):
        return kept[fwd_slot, :, cols].astype(F32)

    def bwd_in(cols):
        return kept[bwd_slot, :, cols].astype(F32)

    def rows_of(index):
        return pl.ds(pl.multiple_of(index * own_rows, own_rows), own_rows)

    def block_of(index):
        return pl.ds(pl.multiple_of(index * block, block), block)

    def gather_copy(which, target, index, hop):
        bit = side if hop == 0 else 1
        place = rows_of(index)
        return pltpu.make_async_remote_copy(
            src_ref=target.at[place],
            dst_ref=target.at[place],
            send_sem=gather_send.at[which, hop],
            recv_sem=gather_recv.at[which, hop],
            device_id={"row": flipped(row, bit)},
            device_id_type=MESH,
        )

    def start_copy(which):
        if which == 0:
            return pltpu.make_async_copy(upstream, up_all.at[rows_of(row)], start_sem.at[0])
        return pltpu.make_async_copy(stash_inputs, kept, start_sem.at[1])

    def slope_copy(unit):
        cols = pl.ds(pl.multiple_of(chunk_of(unit) * width, width), width)
        slot = lax.rem(unit, 2)
        return pltpu.make_async_copy(
            stash_hidden.at[:, :, cols], slopes.at[slot], slope_sem.at[slot]
        )

    def clear(cols):
        acc[:, cols] = jnp.zeros((tokens, cols.size), F32)

    def first_copy(index, start):
        slot = lax.rem(index, 2)

        place = pl.ds(pl.multiple_of(chunk_of(index) * width, width), width)

        @pl.when(backward(index))
        def _():
            copy = pltpu.make_async_copy(w_out.at[place], first_out.at[slot], first_sem.at[slot])
            copy.start() if start else copy.wait()

        @pl.when(jnp.logical_not(backward(index)))
        def _():
            copy = pltpu.make_async_copy(w_in.at[:, place], first_in.at[slot], first_sem.at[slot])
            copy.start() if start else copy.wait()

    def second_copy(index, start):
        slot = lax.rem(index, 2)

        place = pl.ds(pl.multiple_of(chunk_of(index) * width, width), width)

        @pl.when(backward(index))
        def _():
            copy = pltpu.make_async_copy(w_in.at[:, place], second_in.at[slot], second_sem.at[slot])
            copy.start() if start else copy.wait()

        @pl.when(jnp.logical_not(backward(index)))
        def _():
            copy = pltpu.make_async_copy(w_out.at[place], second_out.at[slot], second_sem.at[slot])
            copy.start() if start else copy.wait()

    start_copy(0).start()
    first_copy(jnp.int32(0), True)
    start_copy(1).start()
    slope_copy(jnp.int32(0)).start()
    first_copy(jnp.int32(1), True)
    second_copy(jnp.int32(0), True)
    start_copy(0).wait()
    gather_copy(0, up_all, row, 0).start()
    gather_copy(0, up_all, row, 1).start()

    lane = lax.broadcasted_iota(jnp.int32, (own_rows, LANE), 1)

    def packed(columns):
        values = jnp.zeros((own_rows, LANE), F32)
        for place, column in enumerate(columns):
            values = jnp.where(lane == place, column, values)
        return values

    def stat_copy(which, away):
        return pltpu.make_async_remote_copy(
            src_ref=stat_sent.at[which],
            dst_ref=stat_got.at[which, away - 1],
            send_sem=stat_send.at[which, away - 1],
            recv_sem=stat_recv.at[which, away - 1],
            device_id={"col": (col + away) % n},
            device_id_type=MESH,
        )

    def summed(which):
        values = stat_sent[which]
        for away in range(1, n):
            stat_copy(which, away).wait_recv()
            values = values + stat_got[which, away - 1]
        return values

    def reduced(source):
        def one(step, sums):
            cols = pl.ds(pl.multiple_of(step * strip, strip), strip)
            values = source(cols)
            return tuple(
                s + jnp.sum(v, axis=1, keepdims=True) for s, v in zip(sums, values, strict=True)
            )

        zero = jnp.zeros((own_rows, 1), F32)
        return lax.fori_loop(0, features // strip, one, (zero,) * 2)

    def moments(read):
        def source(cols):
            values = read(cols)
            return values, values * values

        return reduced(source)

    def scale_of(total_sum, squares):
        mean = total_sum * inverse
        return mean, lax.rsqrt(squares * inverse - mean * mean + EPSILON)

    def normalize(cols):
        hat = (fwd_in(cols) - stats[:, 0:1]) * stats[:, 1:2]
        normed_all[rows_of(row), cols] = (hat * gain[:, cols]).astype(BF16)

    def forward_sums():
        start_copy(1).wait()
        stat_sent[0] = packed(moments(fwd_in) + moments(bwd_in))
        for away in range(1, n):
            stat_copy(0, away).start()

    def forward_norm():
        sums = summed(0)
        stats[...] = packed(
            scale_of(sums[:, 0:1], sums[:, 1:2]) + scale_of(sums[:, 2:3], sums[:, 3:4])
        )
        strips(features, strip, normalize)
        gather_copy(1, normed_all, row, 0).start()
        gather_copy(1, normed_all, row, 1).start()

    def pass_on(which, target):
        far = flipped(row, side)
        gather_copy(which, target, far, 0).wait_recv()
        gather_copy(which, target, far, 2).start()

    def gathered_near(which, target):
        gather_copy(which, target, flipped(row, 1), 1).wait_recv()

    def gathered_far(which, target):
        gather_copy(which, target, flipped(flipped(row, 1), side), 2).wait_recv()
        for hop in range(3):
            gather_copy(which, target, row, hop).wait_send()

    def neighbour(way):
        return jnp.minimum(col + 1, last) if way == 0 else jnp.maximum(col - 1, 0)

    def place_in_line(way):
        return col if way == 0 else last - col

    def sum_copy(way, index, hop, target):
        return pltpu.make_async_remote_copy(
            src_ref=part.at[lax.rem(index, n), block_of(target)],
            dst_ref=moved.at[way, lax.rem(index, 3), hop],
            send_sem=sum_send.at[way, lax.rem(index + hop, 2), hop],
            recv_sem=sum_recv.at[way, lax.rem(index, 3), hop],
            device_id={"col": neighbour(way)},
            device_id_type=MESH,
        )

    def spread_copy(way, index, hop, origin):
        slot = lax.rem(index, n + 1)
        return pltpu.make_async_remote_copy(
            src_ref=held.at[slot, block_of(origin)],
            dst_ref=held.at[slot, block_of(origin)],
            send_sem=spread_send.at[way, lax.rem(index + hop, 2), hop],
            recv_sem=spread_recv.at[way, lax.rem(index, 3), hop],
            device_id={"col": neighbour(way)},
            device_id_type=MESH,
        )

    def valid(index):
        return jnp.logical_and(index >= 0, index < queue)

    def sum_target(way, hop):
        at = last - hop + place_in_line(way)
        return at if way == 0 else last - at

    def spread_origin(way, hop):
        return col - hop if way == 0 else col + hop

    def sum_here(way, index, hop):
        at = place_in_line(way)
        return valid(index) & (at <= hop) & (at < last)

    def spread_here(way, index, hop):
        at = place_in_line(way)
        return valid(index) & (at >= hop)

    def sum_step(index, hop):
        for way in range(2):

            @pl.when(sum_here(way, index, hop))
            def _():
                target = sum_target(way, hop)
                if hop > 0:

                    @pl.when(place_in_line(way) > 0)
                    def _():
                        sum_copy(way, index, hop - 1, target).wait_recv()
                        slot = lax.rem(index, n)
                        mine = part[slot, block_of(target)].astype(F32)
                        more = moved[way, lax.rem(index, 3), hop - 1].astype(F32)
                        part[slot, block_of(target)] = (mine + more).astype(BF16)

                sum_copy(way, index, hop, target).start()

    def sum_sent(index, hop):
        for way in range(2):

            @pl.when(sum_here(way, index, hop))
            def _():
                sum_copy(way, index, hop, sum_target(way, hop)).wait_send()

    def spread_step(index, hop):
        for way in range(2):

            @pl.when(spread_here(way, index, hop))
            def _():
                origin = spread_origin(way, hop)
                if hop > 0:
                    spread_copy(way, index, hop - 1, origin).wait_recv()

                @pl.when(place_in_line(way) < last)
                def _():
                    spread_copy(way, index, hop, origin).start()

    def spread_sent(index, hop):
        for way in range(2):

            @pl.when(spread_here(way, index, hop) & (place_in_line(way) < last))
            def _():
                spread_copy(way, index, hop, spread_origin(way, hop)).wait_send()

    def spread_done(index):
        for way in range(2):
            origin = spread_origin(way, last)

            @pl.when(place_in_line(way) == last)
            def _():
                spread_copy(way, index, n - 2, origin).wait_recv()

    def activate(index):
        slot = lax.rem(index, n)
        out_slot = lax.rem(index, n + 1)
        for way in range(2):

            @pl.when(place_in_line(way) > 0)
            def _():
                sum_copy(way, index, n - 2, col).wait_recv()

        total[...] = part[slot, block_of(col)].astype(F32)
        for way in range(2):

            @pl.when(place_in_line(way) > 0)
            def _():
                total[...] += moved[way, lax.rem(index, 3), n - 2].astype(F32)

        tile = STRIP if width % STRIP == 0 else LANE

        @pl.when(backward(index))
        def _():
            for at in range(0, width, tile):
                slot_of = lax.rem(index, 2)
                before = slopes[slot_of, 0, :, at : at + tile].astype(F32)
                for other in range(1, slopes.shape[1]):
                    before = jnp.where(
                        bwd_slot == other,
                        slopes[slot_of, other, :, at : at + tile].astype(F32),
                        before,
                    )
                held[out_slot, block_of(col), at : at + tile] = (
                    total[:, at : at + tile] * gelu_slope(before)
                ).astype(BF16)

        @pl.when(jnp.logical_not(backward(index)))
        def _():
            for at in range(0, width, tile):
                cols = pl.ds(pl.multiple_of(chunk_of(index) * width + at, tile), tile)
                values = total[:, at : at + tile] + b_in[:, cols]
                saved[:, cols] = values.astype(BF16)
                held[out_slot, block_of(col), at : at + tile] = gelu_value(values).astype(BF16)

    both_last = (((1,), (1,)), ((), ()))
    both_inner = (((1,), (0,)), ((), ()))

    def first_product(index):
        slot = lax.rem(index, 2)
        out_slot = lax.rem(index, n)
        tile = 256 if width % 256 == 0 else width

        @pl.when(backward(index))
        def _():
            for at in range(0, width, tile):
                part[out_slot, :, at : at + tile] = lax.dot_general(
                    up_all[...], first_out[slot, at : at + tile, :], both_last,
                    preferred_element_type=F32,
                ).astype(BF16)

        @pl.when(jnp.logical_not(backward(index)))
        def _():
            for at in range(0, width, tile):
                part[out_slot, :, at : at + tile] = lax.dot_general(
                    normed_all[...], first_in[slot, :, at : at + tile], both_inner,
                    preferred_element_type=F32,
                ).astype(BF16)

    def second_product(index):
        slot = lax.rem(index, 2)
        in_slot = lax.rem(index, n + 1)
        tile = min(256, features)
        group = 2 if features % (2 * tile) == 0 else 1

        @pl.when(backward(index))
        def _():
            @pl.loop(0, features // (tile * group))
            def _(step):
                for k in range(group):
                    at = pl.ds(pl.multiple_of((step * group + k) * tile, tile), tile)
                    acc[:, at] += lax.dot_general(
                        held[in_slot], second_in[slot, at, :], both_last,
                        preferred_element_type=F32,
                    )

        @pl.when(jnp.logical_not(backward(index)))
        def _():
            @pl.loop(0, features // (tile * group))
            def _(step):
                for k in range(group):
                    at = pl.ds(pl.multiple_of((step * group + k) * tile, tile), tile)
                    acc[:, at] += lax.dot_general(
                        held[in_slot], second_out[slot, :, at], both_inner,
                        preferred_element_type=F32,
                    )

    def half_copy(which, k, p):
        return pltpu.make_async_remote_copy(
            src_ref=half_sent.at[k, p],
            dst_ref=half_got.at[k, p],
            send_sem=half_send.at[which, k, p],
            recv_sem=half_recv.at[which, k, p],
            device_id={"row": flipped(row, 1)},
            device_id_type=MESH,
        )

    def side_copy(which, p):
        return pltpu.make_async_remote_copy(
            src_ref=side_sent.at[p],
            dst_ref=side_got.at[p],
            send_sem=side_send.at[which, p],
            recv_sem=side_recv.at[which, p],
            device_id={"row": flipped(row, side)},
            device_id_type=MESH,
        )

    def final_copy(which, p):
        target = grad_recv if which == 0 else act_recv
        away = sections - 1 if which == 0 else 1
        cols = pl.ds(p * piece, piece)
        return pltpu.make_async_remote_copy(
            src_ref=final.at[which, :, cols],
            dst_ref=target.at[:, cols],
            send_sem=final_send.at[which, p],
            recv_sem=final_recv.at[which, p],
            device_id={"section": (section + away) % sections},
            device_id_type=MESH,
        )

    def fold_near(which):
        if which == 1:
            pl.semaphore_wait(half_free, 1)
        for k in (1, 0):
            index = flipped_by(row, 1 + side * k)
            for p in range(pieces):
                cols = pl.ds(p * piece, piece)
                half_sent[k, p] = acc[rows_of(index), cols].astype(BF16)
                half_copy(which, k, p).start()

    def fold_far(which):
        if which == 1:
            pl.semaphore_wait(side_free, 1)
        far = flipped(row, side)
        for p in range(pieces):
            half_copy(which, 1, p).wait_recv()
            cols = pl.ds(p * piece, piece)
            side_sent[p] = (acc[rows_of(far), cols] + half_got[1, p].astype(F32)).astype(BF16)
            side_copy(which, p).start()

    def backward_own():
        for p in range(pieces):
            half_copy(0, 0, p).wait_recv()
            cols = pl.ds(p * piece, piece)
            own[:, cols] = acc[rows_of(row), cols] + half_got[0, p].astype(F32)
        for k in range(2):
            for p in range(pieces):
                half_copy(0, k, p).wait_send()
        pl.semaphore_signal(half_free, 1, device_id={"row": flipped(row, 1)}, device_id_type=MESH)
        strips(features, strip, clear)

    def backward_hat(cols):
        return (bwd_in(cols) - stats[:, 2:3]) * stats[:, 3:4]

    def backward_sums():
        for p in range(pieces):
            side_copy(0, p).wait_recv()
            cols = pl.ds(p * piece, piece)
            own[:, cols] = (own[:, cols] + side_got[p].astype(F32)) * gain[:, cols]
        for p in range(pieces):
            side_copy(0, p).wait_send()
        pl.semaphore_signal(
            side_free, 1, device_id={"row": flipped(row, side)}, device_id_type=MESH
        )

        def source(cols):
            scaled = own[:, cols]
            return scaled, scaled * backward_hat(cols)

        stat_sent[1] = packed(reduced(source))
        for away in range(1, n):
            stat_copy(1, away).start()

    def backward_end():
        sums = summed(1) * inverse
        stats[...] = packed((stats[:, 0:1], stats[:, 1:2], stats[:, 2:3], stats[:, 3:4], sums[:, 0:1], sums[:, 1:2]))

        def finish(cols):
            values = own[:, cols] - stats[:, 4:5] - backward_hat(cols) * stats[:, 5:6]
            final[0, :, cols] = (
                up_all[rows_of(row), cols].astype(F32) + stats[:, 3:4] * values
            ).astype(BF16)

        strips(features, strip, finish)
        for p in range(pieces):
            final_copy(0, p).start()

    turn = 2 * n - 2
    steps = queue + turn
    middle = chunks - 1 + turn

    def at_step(m, step, *actions):
        @pl.when(m == step)
        def _():
            for action in actions:
                action()

    def step(m, carry):
        second = m - turn
        ready = m - last

        for way in range(2):

            @pl.when((m >= 2) & (place_in_line(way) < last))
            def _():
                pl.semaphore_wait(credit.at[way], 1)

        @pl.when(m + 2 < queue)
        def _():
            first_copy(m + 2, True)

        @pl.when((second >= 0) & (second + 1 < queue))
        def _():
            second_copy(second + 1, True)

        @pl.when((ready >= 0) & (ready + 1 < chunks))
        def _():
            slope_copy(ready + 1).start()

        for hop in range(n - 1):
            sum_step(m - hop, hop)

        @pl.when((ready >= 0) & (ready < chunks))
        def _():
            slope_copy(ready).wait()

        @pl.when(valid(ready))
        def _():
            activate(ready)

        for hop in range(n - 1):
            spread_step(ready - hop, hop)

        at_step(m, 6, lambda: pass_on(1, normed_all))
        at_step(
            m, chunks - 1,
            lambda: gathered_near(1, normed_all), lambda: gathered_far(1, normed_all),
        )
        at_step(m, middle + 1, lambda: fold_far(0), backward_own)
        at_step(m, middle + 3, backward_sums)
        at_step(m, middle + 4, backward_end)

        @pl.when(valid(second))
        def _():
            spread_done(second)
            second_copy(second, False)
            second_product(second)

        at_step(m, middle, lambda: fold_near(0))

        for hop in range(n - 1):
            sum_sent(m - 1 - hop, hop)
            spread_sent(m - 1 - last - hop, hop)

        @pl.when(m + 1 < queue)
        def _():
            first_copy(m + 1, False)
            first_product(m + 1)

        for way in range(2):

            @pl.when((m < steps - 2) & (place_in_line(way) > 0))
            def _():
                pl.semaphore_signal(
                    credit.at[way], 1, device_id={"col": neighbour(1 - way)}, device_id_type=MESH
                )

        return carry

    forward_sums()
    strips(features, strip, clear)
    forward_norm()
    gathered_near(0, up_all)
    pass_on(0, up_all)
    gathered_far(0, up_all)
    first_copy(jnp.int32(0), False)
    first_product(jnp.int32(0))
    lax.fori_loop(0, steps, step, 0)

    fold_near(1)
    fold_far(1)
    for p in range(pieces):
        half_copy(1, 0, p).wait_recv()
        cols = pl.ds(p * piece, piece)
        own[:, cols] = acc[rows_of(row), cols] + (
            half_got[0, p].astype(F32) + b_out[:, cols] + fwd_in(cols)
        )
    for p in range(pieces):
        side_copy(1, p).wait_recv()
        cols = pl.ds(p * piece, piece)
        final[1, :, cols] = (own[:, cols] + side_got[p].astype(F32)).astype(BF16)
        final_copy(1, p).start()
    for p in range(pieces):
        side_copy(1, p).wait_send()
        for k in range(2):
            half_copy(1, k, p).wait_send()
    for which in range(2):
        for away in range(1, n):
            stat_copy(which, away).wait_send()
        for p in range(pieces):
            final_copy(which, p).wait()


def cut_count(features):
    return max(p for p in range(1, 9) if features % (p * LANE) == 0)


def whole_layer(shape, *operands):
    n, ranks, sections = shape["col"], shape["row"], shape["section"]
    upstream, w_in = operands[6], operands[7]
    own_rows, features = upstream.shape
    depth = operands[4].shape[0]
    hidden_units = w_in.shape[1]
    tokens = own_rows * ranks
    block = tokens // n
    width = WIDTH if n <= 8 else 256
    pieces = cut_count(features)
    dma = pltpu.SemaphoreType.DMA
    in_vmem = pl.BlockSpec(memory_space=pltpu.VMEM)
    anywhere = pl.BlockSpec(memory_space=pl.ANY)
    scratch = [
        pltpu.VMEM((tokens, features), BF16),
        pltpu.VMEM((tokens, features), BF16),
        pltpu.VMEM((tokens, features), F32),
        pltpu.VMEM((2, features, width), BF16),
        pltpu.VMEM((2, width, features), BF16),
        pltpu.VMEM((2, features, width), BF16),
        pltpu.VMEM((2, width, features), BF16),
        pltpu.VMEM((n, tokens, width), BF16),
        pltpu.VMEM((2, 3, n - 1, block, width), BF16),
        pltpu.VMEM((n + 1, tokens, width), BF16),
        pltpu.VMEM((block, width), F32),
        pltpu.VMEM((own_rows, features), F32),
        pltpu.VMEM((own_rows, LANE), F32),
        pltpu.VMEM((2, own_rows, LANE), F32),
        pltpu.VMEM((2, n - 1, own_rows, LANE), F32),
        pltpu.VMEM((2, pieces, own_rows, features // pieces), BF16),
        pltpu.VMEM((2, pieces, own_rows, features // pieces), BF16),
        pltpu.VMEM((pieces, own_rows, features // pieces), BF16),
        pltpu.VMEM((pieces, own_rows, features // pieces), BF16),
        pltpu.VMEM((2, own_rows, features), BF16),
        pltpu.VMEM((depth, own_rows, features), BF16),
        pltpu.VMEM((2, depth, block, width), BF16),
        dma((2,)),
        dma((2,)),
        dma((2,)),
        dma((2,)),
        dma((2, 2, n - 1)),
        dma((2, 3, n - 1)),
        dma((2, 2, n - 1)),
        dma((2, 3, n - 1)),
        dma((2, 3)),
        dma((2, 3)),
        dma((2, n - 1)),
        dma((2, n - 1)),
        dma((2, 2, pieces)),
        dma((2, 2, pieces)),
        dma((2, pieces)),
        dma((2, pieces)),
        dma((2, pieces)),
        dma((2, pieces)),
        pltpu.SemaphoreType.REGULAR((2,)),
        pltpu.SemaphoreType.REGULAR,
        pltpu.SemaphoreType.REGULAR,
    ]
    return pl.pallas_call(
        functools.partial(kernel, n, ranks, sections, width, pieces),
        out_shape=(
            jax.ShapeDtypeStruct((own_rows, features), BF16),
            jax.ShapeDtypeStruct((own_rows, features), BF16),
            jax.ShapeDtypeStruct((block, hidden_units), BF16),
        ),
        in_specs=[pl.BlockSpec(memory_space=pltpu.SMEM)] + [in_vmem] * 3 + [anywhere] * 5,
        out_specs=(anywhere, anywhere, in_vmem),
        scratch_shapes=scratch,
        name="layer",
        cost_estimate=pl.CostEstimate(
            flops=8 * tokens * features * hidden_units,
            bytes_accessed=8 * features * hidden_units,
            transcendentals=0,
        ),
        compiler_params=pltpu.CompilerParams(
            collective_id=0, has_side_effects=True, vmem_limit_bytes=67043328
        ),
    )(*operands)


def body(shape, stash_inputs, stash_hidden, grad_in, w_in, b_in, w_out, b_out, ln_gain, plan):
    act, grad, saved = whole_layer(
        shape, plan, b_in, b_out, ln_gain, stash_inputs[0], stash_hidden[0], grad_in[0], w_in[0], w_out[0]
    )
    return (act[None], grad[None], saved[None])


def solution(mesh):
    in_specs = (
        P("section", None, "row", "col"),
        P("section", None, "col", "row"),
        P("section", "row", "col"),
        P("section", "col", "row"),
        P("section", "row"),
        P("section", "row", "col"),
        P("section", "col"),
        P("section", "col"),
        P("section", None),
    )
    out_specs = (P("section", "row", "col"), P("section", "row", "col"), P("section", "col", "row"))
    return jax.shard_map(
        functools.partial(body, dict(mesh.shape)),
        mesh=mesh,
        in_specs=in_specs,
        out_specs=out_specs,
        check_vma=False,
    )
```
